256 devices in a mesh: scene: 2 (over y), cam: 128 (over x, z, core).
Axes of the slice: x: 4, y: 2, z: 16, core: 2. Of those that a mesh axis runs over, the one named last changes fastest.
The devices are a block of a 4x16x16 slice.
Arguments:
- queries: bfloat16 [256, 768, 1024], P(('scene', 'cam')), parts along dimension 0, may hold values from -32 to 32
- keys: bfloat16 [256, 768, 1024], P(('scene', 'cam')), parts along dimension 0, may hold values from -32 to 32
- values: bfloat16 [256, 768, 1024], P(('scene', 'cam')), parts along dimension 0, may hold values from -6 to 6
- residual: bfloat16 [256, 768, 1024], P(('scene', 'cam')), parts along dimension 0, may hold values from -1.5 to 1.5
- w_out: bfloat16 [1024, 1024], replicated, may hold values from -0.1875 to 0.1875
- neighbours: int32 [256, 4], P(('scene', 'cam')), parts along dimension 0, may hold values from 0 to 127, as said below
- band_start: int32 [256, 4], P(('scene', 'cam')), parts along dimension 0, may hold values from 0 to 3
- band_blocks: int32 [256, 4, 6, 2], P(('scene', 'cam')), parts along dimension 0, may hold values from 0 to 2, as said below
- band_count: int32 [256, 4, 6], P(('scene', 'cam')), parts along dimension 0, may hold values from 1 to 2, as said below
Outputs:
- output: bfloat16 [256, 768, 1024], P(('scene', 'cam')), parts along dimension 0
The draws below stay inside these ranges and needn't reach their ends.
There are 2 independent parts, one for each index of `scene`. The reference program is written for one: setup_inputs(seed, part) draws one part's arguments, and reference() takes and returns one part's arrays. A program takes and returns all parts, laid end to end along the dimension named above; an argument that names none is the same for every part. Nothing has to cross between parts.
Inputs may be any that keep to these rules, and one draw needn't show every extreme that they name: `neighbours`: row v lists the views (v + k * 4) mod 128 for k = 1, -1, 2, -2, each once, in an order drawn for each row. `band_blocks`: each list holds 2 different numbers; entries at positions band_count or later are not read. `band_count`: query block 0 of every slot has 2.
All inputs are finite; a program needn't handle non-finite values.
Results may differ from the reference program's by a relative error of at most 0.008.
Values may be sent and summed in bfloat16 or wider, within the bound.
No kernel may reach another device: no remote copies, remote signals or barrier semaphores. Data moves between devices by JAX's collectives and lax.ppermute only.
A program may use at most 128 MiB of HBM per device.

```python
import jax
import jax.numpy as jnp
from jax import lax

D = 1024
HEADS = 16
TOK = 768
MOST = 2
RIGS = 4
VIEWS = 128
QB = 6
WIN = 3


def drawn_pair(key):
    base_key = jax.random.fold_in(key, 17)
    query_key, key_key = jax.random.split(base_key, 2)
    query_draw = 2.0 * jnp.clip(jax.random.normal(query_key, (VIEWS, TOK, D), jnp.float32), -6.0, 6.0)
    key_draw = jnp.clip(jax.random.normal(key_key, (VIEWS, TOK, D), jnp.float32), -6.0, 6.0)
    return (query_draw.astype(jnp.bfloat16), key_draw.astype(jnp.bfloat16))


def draw_queries(key, part):
    return drawn_pair(key)[0]


def draw_keys(key, part):
    return drawn_pair(key)[1]


def draw_neighbours(key, part):
    order_key = jax.random.fold_in(key, 3)
    ranks = jax.random.randint(order_key, (VIEWS, 4), 0, 1 << 20) * 4 + jnp.arange(4, dtype=jnp.int32)[None, :]
    order = jnp.argsort(ranks, axis=1, stable=True)
    offsets = jnp.array([1, -1, 2, -2], dtype=jnp.int32)[order]
    views = jnp.arange(VIEWS, dtype=jnp.int32)[:, None]
    return ((views + offsets * RIGS + 2 * VIEWS) % VIEWS).astype(jnp.int32)


def draw_band_blocks(key, part):
    order_key = jax.random.fold_in(key, 5)
    ranks = jax.random.randint(order_key, (VIEWS, 4, QB, WIN), 0, 1 << 20) * WIN + jnp.arange(WIN, dtype=jnp.int32)
    order = jnp.argsort(ranks, axis=-1, stable=True)
    return order[..., :MOST].astype(jnp.int32)


def draw_band_count(key, part):
    level_key = jax.random.fold_in(key, 7)
    roll_key = jax.random.fold_in(key, 11)
    levels = jax.random.randint(level_key, (VIEWS, 1, 1), 1, 10)
    rolls = jax.random.randint(roll_key, (VIEWS, 4, QB), 0, 10)
    counted = jnp.where(rolls < levels, MOST, 1).astype(jnp.int32)
    return counted.at[:, :, 0].set(MOST)


def plant(values, rng, low, top_value):
    place = [jax.random.randint(jax.random.fold_in(rng, axis), (), 0, length) for axis, length in enumerate(values.shape)]
    main_axis = values.shape.index(max(values.shape))
    neighbour = place[:main_axis] + [(place[main_axis] + 1) % values.shape[main_axis]] + place[main_axis + 1:]
    return values.at[tuple(place)].set(low).at[tuple(neighbour)].set(top_value)


def shard_levels(key, dims, cuts, least, high):
    def one(dim, shards_of):
        draws = jax.random.uniform(jax.random.fold_in(jax.random.fold_in(key, 6), dim), (shards_of,), jnp.float32, least / len(cuts), high / len(cuts))
        return jnp.repeat(jnp.exp(draws), dims[dim] // shards_of).reshape((-1,) + (1,) * (len(dims) - dim - 1))

    level = one(*cuts[0])
    for cut in cuts[1:]:
        level = level * one(*cut)
    return level


def gaussian(stream_key, dims, width, reach, cuts=(), kind=jnp.bfloat16):
    values = width * jax.random.normal(stream_key, dims, jnp.float32)
    if cuts:
        values = values * shard_levels(stream_key, dims, cuts, -0.22, 0.18)
    return jnp.clip(values, -reach, reach).astype(kind)


def setup_inputs(seed: int = 0, part: int = 0) -> dict:
    key_list = jax.random.split(jax.random.key(seed), 10)
    part_keys = jax.random.split(jax.random.fold_in(key_list[9], part), 10)
    queries = draw_queries(jax.random.fold_in(jax.random.fold_in(key_list[9], part), 71), part)
    keys = draw_keys(jax.random.fold_in(jax.random.fold_in(key_list[9], part), 71), part)
    values = gaussian(part_keys[2], (VIEWS, TOK, D), 1.0, 6.0, ((0, 128),))
    residual = gaussian(part_keys[3], (VIEWS, TOK, D), 0.25, 1.5, ((0, 128),))
    w_out = gaussian(key_list[4], (D, D), D ** -0.5, 0.1875)
    neighbours = draw_neighbours(jax.random.fold_in(jax.random.fold_in(key_list[9], part), 71), part)
    band_start = plant(jax.random.randint(part_keys[6], (VIEWS, 4), 0, QB - WIN + 1), jax.random.fold_in(part_keys[6], 1), 0, QB - WIN).astype(jnp.int32)
    band_blocks = draw_band_blocks(jax.random.fold_in(jax.random.fold_in(key_list[9], part), 71), part)
    band_count = draw_band_count(jax.random.fold_in(jax.random.fold_in(key_list[9], part), 71), part)
    return dict(queries=queries, keys=keys, values=values, residual=residual, w_out=w_out, neighbours=neighbours, band_start=band_start, band_blocks=band_blocks, band_count=band_count)


def reference(queries, keys, values, residual, w_out, neighbours, band_start, band_blocks, band_count):
    cameras, tokens, model_width = queries.shape
    qblocks = band_count.shape[2]
    most_blocks = band_blocks.shape[3]
    block_len = tokens // qblocks
    head_dim = model_width // HEADS
    score_scale = 1.0 / (head_dim ** 0.5)
    key_tiles = keys.reshape(cameras, qblocks, block_len, model_width)
    value_tiles = values.reshape(cameras, qblocks, block_len, model_width)

    def one_view(view_index):
        near_cams = neighbours[view_index]
        absolute = band_start[view_index][:, None, None] + band_blocks[view_index]
        near_keys = key_tiles[near_cams[:, None, None], absolute]
        near_values = value_tiles[near_cams[:, None, None], absolute]
        near_keys = jnp.transpose(near_keys, (1, 0, 2, 3, 4)).reshape(qblocks, 4 * most_blocks * block_len, model_width)
        near_values = jnp.transpose(near_values, (1, 0, 2, 3, 4)).reshape(qblocks, 4 * most_blocks * block_len, model_width)
        all_keys = jnp.concatenate([key_tiles[view_index], near_keys], axis=1).reshape(qblocks, -1, HEADS, head_dim)
        all_values = jnp.concatenate([value_tiles[view_index], near_values], axis=1).reshape(qblocks, -1, HEADS, head_dim)
        live_slots = jnp.arange(most_blocks, dtype=jnp.int32)[None, None, :] < band_count[view_index][:, :, None]
        live_slots = jnp.repeat(jnp.transpose(live_slots, (1, 0, 2)), block_len, axis=2).reshape(qblocks, -1)
        visible = jnp.concatenate([jnp.ones((qblocks, block_len), dtype=bool), live_slots], axis=1)
        query_tiles = queries[view_index].reshape(qblocks, block_len, HEADS, head_dim)
        scores = jnp.einsum("gqhd,gkhd->ghqk", query_tiles.astype(jnp.float32), all_keys.astype(jnp.float32)) * score_scale
        scores = jnp.where(visible[:, None, None, :], scores, -jnp.inf)
        row_max = jnp.max(scores, axis=-1, keepdims=True)
        expo_scores = jnp.exp(scores - row_max)
        weights = (expo_scores / jnp.sum(expo_scores, axis=-1, keepdims=True)).astype(jnp.bfloat16)
        attended = jnp.einsum("ghqk,gkhd->gqhd", weights.astype(jnp.float32), all_values.astype(jnp.float32))
        attended = attended.astype(jnp.bfloat16).reshape(tokens, model_width)
        projected = jnp.dot(attended, w_out, preferred_element_type=jnp.float32)
        return (residual[view_index].astype(jnp.float32) + projected).astype(jnp.bfloat16)

    return lax.map(one_view, jnp.arange(cameras, dtype=jnp.int32))
```

```python
import functools
import math

import jax
import jax.numpy as jnp
from jax import lax
from jax.experimental import pallas as pl
from jax.experimental.pallas import tpu as pltpu
from jax.sharding import PartitionSpec as P


HEADS = 16
DEAD = 1e30


def passed_along(block, axis, distance):
    devices = range(lax.axis_size(axis))
    route = [((i - distance) % len(devices), i) for i in devices]
    return lax.ppermute(block, axis, route)


def head_masks(rows, lanes, head_dim):
    lane = lax.broadcasted_iota(jnp.int32, (rows, lanes), 1)
    return lane < head_dim


def tile_scores(q2, key_list, dead_list, mix):
    scores = []
    top = None
    for keys, dead in zip(key_list, dead_list):
        s = lax.dot_general(
            q2, keys, (((1,), (1,)), ((), ())), preferred_element_type=jnp.float32
        )
        scores.append(s)
        seen = s if dead is None else s - dead
        top = seen if top is None else jnp.maximum(top, seen)
    row_max = jnp.max(top, axis=-1, keepdims=True)
    if mix is not None:
        row_max = jnp.maximum(row_max, mix)
    return scores, row_max


def weighted(scores, row_max, dead_list, value_list, factor):
    _, block_len = scores[0].shape
    ones = jnp.ones((block_len, value_list[0].shape[1]), jnp.bfloat16)
    probs = []
    for s, dead in zip(scores, dead_list):
        level = row_max if dead is None else row_max + dead
        probs.append(jnp.exp2((s - level) * factor).astype(jnp.bfloat16))
    weights = jnp.concatenate(probs, axis=1)
    values = jnp.concatenate(
        [jnp.concatenate([v, ones], axis=1) for v in value_list], axis=0
    )
    return jnp.dot(weights, values, preferred_element_type=jnp.float32)


def near_kernel(
    factor, qblocks, block_len, head_dim,
    index_ref, dead_ref, q_ref, k_ref, v_ref, kp_ref, vp_ref, kn_ref, vn_ref,
    acc_ref, top_ref, sum_ref,
):
    pair = 2 * head_dim
    low = head_masks(block_len, pair, head_dim)

    def one_block(b, carry):
        base = pl.multiple_of(b * block_len, block_len)
        q = q_ref[pl.ds(base, block_len), :]
        zero = jnp.zeros_like(q)
        q2 = jnp.concatenate([jnp.where(low, q, zero), jnp.where(low, zero, q)], axis=0)
        keys = [k_ref[pl.ds(base, block_len), :]]
        values = [v_ref[pl.ds(base, block_len), :]]
        dead = [None]
        for source, (kr, vr) in enumerate(((kp_ref, vp_ref), (kn_ref, vn_ref))):
            for m in range(2):
                at = pl.multiple_of(index_ref[b, source * 2 + m] * block_len, block_len)
                keys.append(kr[pl.ds(at, block_len), :])
                values.append(vr[pl.ds(at, block_len), :])
                dead.append(dead_ref[b, source] if m else None)
        scores, row_max = tile_scores(q2, keys, dead, None)
        out = weighted(scores, row_max, dead, values, factor)
        top2 = jnp.broadcast_to(row_max, (2 * block_len, pair))
        acc_ref[pl.ds(base, block_len), :] = jnp.where(low, out[:block_len, :pair], out[block_len:, :pair])
        sum_ref[pl.ds(base, block_len), :] = jnp.where(low, out[:block_len, pair:], out[block_len:, pair:])
        top_ref[pl.ds(base, block_len), :] = jnp.where(low, top2[:block_len], top2[block_len:])
        return carry

    lax.fori_loop(0, qblocks, one_block, 0, unroll=True)


def far_kernel(
    factor, qblocks, block_len, head_dim, steps, first,
    index_ref, dead_ref, q_ref, kp_ref, vp_ref, kn_ref, vn_ref,
    acc_ref, top_ref, sum_ref, w_ref, base_ref, out_ref, attended_ref,
):
    pair = 2 * head_dim
    low = head_masks(block_len, pair, head_dim)
    step = pl.program_id(0)

    def one_block(b, carry):
        base = pl.multiple_of(b * block_len, block_len)
        q = q_ref[pl.ds(base, block_len), :]
        zero = jnp.zeros_like(q)
        q2 = jnp.concatenate([jnp.where(low, q, zero), jnp.where(low, zero, q)], axis=0)
        keys, values, dead = [], [], []
        for source, (kr, vr) in enumerate(((kp_ref, vp_ref), (kn_ref, vn_ref))):
            for m in range(2):
                at = pl.multiple_of(index_ref[b, source * 2 + m] * block_len, block_len)
                keys.append(kr[pl.ds(at, block_len), :])
                values.append(vr[pl.ds(at, block_len), :])
                dead.append(dead_ref[b, source] if m else None)
        top = top_ref[pl.ds(base, block_len), :]
        start = jnp.concatenate([top[:, :1], top[:, head_dim:head_dim + 1]], axis=0)
        scores, row_max = tile_scores(q2, keys, dead, start)
        out = weighted(scores, row_max, dead, values, factor)
        top2 = jnp.broadcast_to(row_max, (2 * block_len, pair))
        now = jnp.where(low, top2[:block_len], top2[block_len:])
        fade = jnp.exp2((top - now) * factor)
        acc = acc_ref[pl.ds(base, block_len), :] * fade + jnp.where(
            low, out[:block_len, :pair], out[block_len:, :pair])
        total = sum_ref[pl.ds(base, block_len), :] * fade + jnp.where(
            low, out[:block_len, pair:], out[block_len:, pair:])
        attended_ref[step, pl.ds(base, block_len), :] = (acc / total).astype(jnp.bfloat16)
        return carry

    lax.fori_loop(0, qblocks, one_block, 0, unroll=True)

    @pl.when(step == steps - 1)
    def _():
        def project(b, carry):
            base = pl.multiple_of(b * block_len, block_len)
            rows = jnp.concatenate(
                [attended_ref[i, pl.ds(base, block_len), :] for i in range(steps)], axis=1
            )
            out_ref[pl.ds(base, block_len), :] = (
                base_ref[pl.ds(base, block_len), :].astype(jnp.float32)
                + jnp.dot(rows, w_ref[first:first + steps * pair, :], preferred_element_type=jnp.float32)
            ).astype(out_ref.dtype)
            return carry

        lax.fori_loop(0, qblocks, project, 0)


def attend_near(index, dead, q, k, v, kp, vp, kn, vn, qblocks, head_dim):
    tokens, width = q.shape
    block_len = tokens // qblocks
    pair = 2 * head_dim
    factor = math.log2(math.e) / math.sqrt(head_dim)
    column = lambda g, *_: (0, g)
    spec = pl.BlockSpec((tokens, pair), column)
    shape = jax.ShapeDtypeStruct((tokens, width), jnp.float32)
    keys_seen = 5 * block_len
    return pl.pallas_call(
        functools.partial(near_kernel, factor, qblocks, block_len, head_dim),
        grid_spec=pltpu.PrefetchScalarGridSpec(
            num_scalar_prefetch=2,
            grid=(width // pair,),
            in_specs=[spec] * 7,
            out_specs=[spec] * 3,
        ),
        out_shape=[shape] * 3,
        name="near",
        cost_estimate=pl.CostEstimate(
            flops=8 * tokens * keys_seen * width, bytes_accessed=7 * tokens * width * 2 + 12 * tokens * width,
            transcendentals=tokens * keys_seen * (width // head_dim)),
        compiler_params=pltpu.CompilerParams(vmem_limit_bytes=40 * 2**20),
    )(index, dead, q, k, v, kp, vp, kn, vn)


def attend_far(
    index, dead, q, kp, vp, kn, vn, acc, top, total, w, base, first, out_dtype, qblocks, head_dim
):
    tokens, width = q.shape
    block_len = tokens // qblocks
    pair = 2 * head_dim
    chunk = vp.shape[1]
    steps = chunk // pair
    factor = math.log2(math.e) / math.sqrt(head_dim)
    offset = first // pair
    shifted = lambda g, *_: (0, g + offset)
    local = lambda g, *_: (0, g)
    whole = lambda g, *_: (0, 0)
    window = vp.shape[0]
    carry = pl.BlockSpec((tokens, pair), shifted)
    keys_seen = 4 * block_len
    return pl.pallas_call(
        functools.partial(
            far_kernel, factor, qblocks, block_len, head_dim, steps, first),
        grid_spec=pltpu.PrefetchScalarGridSpec(
            num_scalar_prefetch=2,
            grid=(steps,),
            in_specs=[
                carry,
                pl.BlockSpec((window, pair), shifted),
                pl.BlockSpec((window, pair), local),
                pl.BlockSpec((window, pair), shifted),
                pl.BlockSpec((window, pair), local),
                carry, carry, carry,
                pl.BlockSpec((width, width), whole),
                pl.BlockSpec((tokens, width), whole),
            ],
            out_specs=pl.BlockSpec((tokens, width), whole),
            scratch_shapes=[pltpu.VMEM((steps, tokens, pair), jnp.bfloat16)],
        ),
        out_shape=jax.ShapeDtypeStruct((tokens, width), out_dtype),
        name="far",
        cost_estimate=pl.CostEstimate(
            flops=8 * tokens * keys_seen * chunk + 2 * tokens * chunk * width,
            bytes_accessed=14 * tokens * chunk + 10 * tokens * width,
            transcendentals=tokens * keys_seen * (chunk // head_dim)),
        compiler_params=pltpu.CompilerParams(vmem_limit_bytes=40 * 2**20),
    )(index, dead, q, kp, vp, kn, vn, acc, top, total, w, base)


def per_device(
    queries, keys, values, residual, w_out, neighbours, band_start, band_blocks, band_count
):
    q, k, v = queries[0], keys[0], values[0]
    tokens, width = q.shape
    qblocks = band_count.shape[2]
    block_len = tokens // qblocks
    window = max(2, qblocks // 2) * block_len
    head_dim = width // HEADS
    cameras = lax.axis_size("cam")
    rigs = cameras // min(32, cameras)
    me = lax.axis_index("cam")
    offsets = (1, -1, 2, -2)
    pair = 2 * head_dim
    early = (width // pair * 5 // 8) * pair
    chunks = ((0, early), (early, width - early))

    k_prev = passed_along(k, "cam", rigs)
    k_next = passed_along(k, "cam", -rigs)
    v_prev = passed_along(v, "cam", rigs)
    v_next = passed_along(v, "cam", -rigs)

    sources = jnp.stack([(me - offset * rigs + 2 * cameras) % cameras for offset in offsets])
    match = (neighbours[0][None, :] == sources[:, None]).astype(jnp.int32)
    starts = jnp.sum(match * band_start[0][None, :], axis=1)
    blocks = jnp.sum(match[:, :, None, None] * band_blocks[0][None], axis=1)
    counts = jnp.sum(match[:, :, None] * band_count[0][None], axis=1)
    live = jnp.arange(2, dtype=jnp.int32)[None, None, :] < counts[:, :, None]
    blocks = jnp.where(live, blocks, blocks[:, :, :1])
    near_blocks = blocks[:2] + starts[:2, None, None]
    as_table = lambda t: jnp.transpose(t, (1, 0, 2)).reshape(qblocks, 4)
    near_index, far_index = as_table(near_blocks), as_table(blocks[2:])
    dead = jnp.where(counts > 1, 0.0, DEAD).astype(jnp.float32)
    near_dead, far_dead = dead[:2].T, dead[2:].T

    ask_prev = passed_along(lax.slice_in_dim(starts, 2, 3), "cam", -rigs)[0]
    ask_next = passed_along(lax.slice_in_dim(starts, 3, 4), "cam", rigs)[0]

    def cut(rows, start, first, size):
        return lax.dynamic_slice(rows, (start * block_len, first), (window, size))

    far_k_prev = passed_along(cut(k_prev, ask_prev, 0, width), "cam", rigs)
    far_k_next = passed_along(cut(k_next, ask_next, 0, width), "cam", -rigs)
    far_v = []
    for (first, size) in chunks:
        far_v.append((
            passed_along(cut(v_prev, ask_prev, first, size), "cam", rigs),
            passed_along(cut(v_next, ask_next, first, size), "cam", -rigs),
        ))

    acc, top, total = attend_near(
        near_index, near_dead, q, k, v, k_prev, v_prev, k_next, v_next, qblocks, head_dim)
    result = residual[0]
    for (first, size), (far_v_prev, far_v_next) in zip(chunks, far_v):
        result = attend_far(
            far_index, far_dead, q, far_k_prev, far_v_prev, far_k_next, far_v_next,
            acc, top, total, w_out, result, first,
            jnp.bfloat16 if first + size == width else jnp.float32, qblocks, head_dim)
    return result[None]


def solution(mesh):
    return jax.shard_map(
        per_device,
        mesh=mesh,
        in_specs=(
            P(("scene", "cam"), None, None),
            P(("scene", "cam"), None, None),
            P(("scene", "cam"), None, None),
            P(("scene", "cam"), None, None),
            P(),
            P(("scene", "cam"), None),
            P(("scene", "cam"), None),
            P(("scene", "cam"), None, None, None),
            P(("scene", "cam"), None, None),
        ),
        out_specs=P(("scene", "cam"), None, None),
        check_vma=False,
    )
```
